32 devices in a mesh: wide: 4 (over y, x), narrow: 8 (over z, core).
Axes of the slice: x: 2, y: 2, z: 4, core: 2. Of those that a mesh axis runs over, the one named last changes fastest.
Arguments:
- right_side: float32 [64, 32768], P(None, ('wide', 'narrow'))
- leaf_blocks: float32 [32768, 1024], P(('wide', 'narrow')), as said below
- factors: float32 [5, 64, 32768], P(None, None, ('wide', 'narrow'))
- leaf_order: int32 [32768], P(('wide', 'narrow')), may hold values from 0 to 32767, as said below
Outputs:
- solution: float32 [64, 32768], P(None, ('wide', 'narrow'))
- residual: float32 [64, 32768], P(None, ('wide', 'narrow'))
The draws below stay inside these ranges and needn't reach their ends.
Inputs may be any that keep to these rules, and one draw needn't show every extreme that they name: `leaf_order`: each aligned block of 1024 entries is a permutation of the indices of that same block. `leaf_blocks`: each leaf block is symmetric.
All inputs are finite; a program needn't handle non-finite values.
Results may differ from the reference program's by a relative error of at most 0.0003.
Values sent between devices are 32-bit elements; how exact they have to be, the bound alone decides.
No kernel may reach another device: no remote copies, remote signals or barrier semaphores. Data moves between devices by JAX's collectives and lax.ppermute only.
A program may use at most 64 MiB of HBM per device.

```python
import jax
import jax.numpy as jnp
from jax import lax

LEAF = 1024
RANK = 64
RHS = 64
ITERS = 2
NLEAF = 32
POINTS = 32768
LEVELS = 5


def scale_of_level(level):
    count = LEAF * 2.0 ** level
    return (0.12 / count) ** 0.5 / (1.0 + (RANK / count) ** 0.5)


def make_factors(key):
    factor_key = jax.random.fold_in(key, 21)
    counts = LEAF * 2.0 ** jnp.arange(LEVELS, dtype=jnp.float32)
    level_scale = jnp.sqrt(0.12 / counts) / (1.0 + jnp.sqrt(RANK / counts))
    values = jax.random.normal(factor_key, (LEVELS, RANK, POINTS), jnp.float32)
    return values * level_scale[:, None, None]


def make_order(key):
    order_key = jax.random.fold_in(key, 31)

    def one_leaf(index):
        return jax.random.permutation(jax.random.fold_in(order_key, index), LEAF).astype(jnp.int32) + index * LEAF
    return jax.vmap(one_leaf)(jnp.arange(NLEAF, dtype=jnp.int32)).reshape(POINTS).astype(jnp.int32)


def draw_right_side(key, part):
    factors = make_factors(key)
    order = make_order(key)
    noise_key = jax.random.fold_in(key, 41)
    coef_key = jax.random.fold_in(key, 42)
    leaf_ids = (jnp.arange(POINTS) // LEAF).astype(jnp.float32)
    aligned = jnp.zeros((RHS, POINTS), jnp.float32)
    for level in range(LEVELS):
        count = NLEAF // 2 ** level
        span = POINTS // count
        level_key = jax.random.fold_in(coef_key, level)
        coef = jax.random.normal(level_key, (count, RHS, RANK), jnp.float32)
        coef = coef * (0.6 / (RANK ** 0.5 * scale_of_level(level)))
        rows = factors[level].reshape(RANK, count, span)
        aligned = aligned + jnp.einsum('brq,qbs->rbs', coef, rows).reshape(RHS, POINTS)
    noise = jax.random.normal(noise_key, (RHS, POINTS), jnp.float32)
    rising = 1.0 + 2.0 * leaf_ids / max(NLEAF - 1, 1)
    values = (noise + aligned) * rising[None, :]
    return jnp.zeros((RHS, POINTS), jnp.float32).at[:, order].set(values)


def draw_leaf_blocks(key, part):
    first = jax.random.fold_in(key, 11)
    second = jax.random.fold_in(key, 12)
    raw = jax.random.normal(first, (NLEAF, LEAF, LEAF), jnp.float32)
    diag = jax.random.uniform(second, (NLEAF, LEAF), jnp.float32, 3.0, 4.5)
    sym = (raw + jnp.swapaxes(raw, 1, 2)) * (0.55 / LEAF ** 0.5)
    eye = jnp.eye(LEAF, dtype=jnp.float32)
    blocks = sym + diag[:, :, None] * eye[None]
    return blocks.reshape(POINTS, LEAF)


def draw_factors(key, part):
    return make_factors(key)


def draw_leaf_order(key, part):
    return make_order(key)


def setup_inputs(seed: int = 0) -> dict:
    key_of = jax.random.split(jax.random.key(seed), 5)
    return {
        "right_side": draw_right_side(jax.random.fold_in(key_of[4], 71), 0),
        "leaf_blocks": draw_leaf_blocks(jax.random.fold_in(key_of[4], 71), 0),
        "factors": draw_factors(jax.random.fold_in(key_of[4], 71), 0),
        "leaf_order": draw_leaf_order(jax.random.fold_in(key_of[4], 71), 0),
    }


HIGH = lax.Precision.HIGHEST


def apply_kernel(vector, leaf_blocks, factors):
    leaves = vector.reshape(RHS, NLEAF, LEAF)
    blocks = leaf_blocks.reshape(NLEAF, LEAF, LEAF)
    result = jnp.einsum("rnl,nlm->rnm", leaves, blocks, precision=HIGH)
    shaped = factors.reshape(LEVELS, RANK, NLEAF, LEAF)
    for level in range(LEVELS):
        width = 2 ** level
        projected = jnp.einsum("rnl,qnl->nrq", leaves, shaped[level], precision=HIGH)
        grouped = projected.reshape(NLEAF // (2 * width), 2, width, RHS, RANK).sum(axis=2)
        sibling = grouped[:, ::-1]
        spread = jnp.broadcast_to(sibling[:, :, None], (NLEAF // (2 * width), 2, width, RHS, RANK))
        spread = spread.reshape(NLEAF, RHS, RANK)
        result = result + jnp.einsum("nrq,qnl->rnl", spread, shaped[level], precision=HIGH)
    return result.reshape(RHS, POINTS)


def reference(right_side, leaf_blocks, factors, leaf_order):
    rhs_leaf = jnp.take(right_side, leaf_order, axis=1)
    solution = jnp.zeros_like(rhs_leaf)
    residual = rhs_leaf
    direction = rhs_leaf
    norm_now = jnp.sum(residual * residual, axis=1)
    for step in range(ITERS):
        image = apply_kernel(direction, leaf_blocks, factors)
        alpha = norm_now / jnp.sum(direction * image, axis=1)
        solution = solution + alpha[:, None] * direction
        residual = residual - alpha[:, None] * image
        if step + 1 < ITERS:
            norm_next = jnp.sum(residual * residual, axis=1)
            direction = residual + (norm_next / norm_now)[:, None] * direction
            norm_now = norm_next
    placed_sol = jnp.zeros_like(right_side).at[:, leaf_order].set(solution)
    placed_res = jnp.zeros_like(right_side).at[:, leaf_order].set(residual)
    return placed_sol, placed_res
```

```python
import jax
import jax.numpy as jnp
from jax import lax
from jax.experimental import pallas as pl
from jax.experimental.pallas import tpu as pltpu
from jax.sharding import PartitionSpec as P

AXES = ("wide", "narrow")
F32 = jnp.float32
BF16 = jnp.bfloat16
TAIL = 8
VMEM = pl.BlockSpec(memory_space=pltpu.VMEM)
HBM = pl.BlockSpec(memory_space=pltpu.HBM)


def dot(a, b):
    return jnp.dot(a, b, preferred_element_type=F32)


def dot_nt(a, b):
    return lax.dot_general(a, b, (((1,), (1,)), ((), ())), preferred_element_type=F32)


def split2(value):
    high = value.astype(BF16)
    return high, (value - high.astype(F32)).astype(BF16)


def split3(value):
    high = value.astype(BF16)
    rest = value - high.astype(F32)
    mid = rest.astype(BF16)
    return high, mid, (rest - mid.astype(F32)).astype(BF16)


def eye_mask(rows, lanes, period):
    row = lax.broadcasted_iota(jnp.int32, (rows, lanes), 0)
    lane = lax.broadcasted_iota(jnp.int32, (rows, lanes), 1)
    return (lane == row) | (lane == row + period)


def to_row(column, lanes):
    rows = column.shape[0]
    row = lax.broadcasted_iota(jnp.int32, (rows, lanes), 0)
    lane = lax.broadcasted_iota(jnp.int32, (rows, lanes), 1)
    return jnp.sum(jnp.where(row == lane, column, 0.0), axis=0, keepdims=True)


def to_column(row, rows):
    lanes = row.shape[1]
    return jnp.sum(jnp.where(eye_mask(rows, lanes, rows), row, 0.0), axis=1, keepdims=True)


def pack_projection(q_hi, q_lo, both, rhs):
    result = dot_nt(q_hi, both) + dot_nt(q_lo, both)
    full = result + pltpu.roll(result, rhs, 1)
    half = full.shape[0] // 2
    lane = lax.broadcasted_iota(jnp.int32, (half, full.shape[1]), 1)
    return jnp.where(lane < rhs, full[:half], full[half:])


def write_message(msg_ref, packed, field, near, rhs):
    lanes = 2 * rhs
    square = jnp.sum(field * field, axis=1, keepdims=True)
    product = jnp.sum(field * near, axis=1, keepdims=True)
    rows = packed.shape[0]
    msg_ref[:rows] = packed
    index = lax.broadcasted_iota(jnp.int32, (TAIL, lanes), 0)
    tail = jnp.where(index == 0, to_row(square, lanes), jnp.where(index == 1, to_row(product, lanes), 0.0))
    msg_ref[rows:] = tail


def near_product(both, field_hi, d_hi, d_lo, rhs):
    wide = dot(both, d_hi)
    return wide[:rhs] + wide[rhs:] + dot(field_hi, d_lo)


def far_product(parts, q_hi, q_lo, rhs):
    stacked = jnp.concatenate(parts, axis=0)
    turned = stacked.T
    half = q_hi.shape[0] // 2
    total = None
    for side in range(2):
        hi, lo = split2(turned[side * rhs:(side + 1) * rhs])
        both = jnp.concatenate([hi, lo], axis=0)
        wide = dot(both, q_hi[side * half:(side + 1) * half])
        part = wide[:rhs] + wide[rhs:] + dot(hi, q_lo[side * half:(side + 1) * half])
        total = part if total is None else total + part
    return total


def first_kernel(order_ref, rs_ref, d_hbm, f_hbm, b_ref, near_ref, msg_ref, dhi_ref, dlo_ref, qhi_ref, qlo_ref,
                 d_ref, f_ref, sems):
    levels, rank, leaf = f_ref.shape
    rhs = rs_ref.shape[0]
    half = rank // 2
    chunk = 256
    chunks = leaf // chunk
    f_copy = pltpu.make_async_copy(f_hbm, f_ref, sems.at[chunks])
    f_copy.start()
    d_copies = []
    for n in range(chunks):
        cols = pl.ds(n * chunk, chunk)
        copy = pltpu.make_async_copy(d_hbm.at[:, cols], d_ref.at[:, cols], sems.at[n])
        copy.start()
        d_copies.append(copy)
    hi, mid, lo = split3(rs_ref[...])
    three = jnp.concatenate([hi, mid, lo], axis=0)
    for n in range(chunks):
        cols = pl.ds(n * chunk, chunk)
        index = lax.broadcasted_iota(jnp.int32, (leaf, chunk), 0)
        onehot = jnp.where(index == order_ref[:, cols], 1.0, 0.0).astype(BF16)
        got = dot(three, onehot)
        b_ref[:, cols] = got[:rhs] + got[rhs:2 * rhs] + got[2 * rhs:]
    field = b_ref[...]
    field_hi, field_lo = split2(field)
    both = jnp.concatenate([field_hi, field_lo], axis=0)
    f_copy.wait()
    for level in range(levels):
        for side in range(2):
            hi, lo = split2(f_ref[level, pl.ds(side * half, half)])
            rows = pl.ds((side * levels + level) * half, half)
            qhi_ref[rows] = hi
            qlo_ref[rows] = lo
    packed = pack_projection(qhi_ref[...], qlo_ref[...], both, rhs)
    for n in range(chunks):
        cols = pl.ds(n * chunk, chunk)
        d_copies[n].wait()
        d_hi, d_lo = split2(d_ref[:, cols])
        dhi_ref[:, cols] = d_hi
        dlo_ref[:, cols] = d_lo
        near_ref[:, cols] = near_product(both, field_hi, d_hi, d_lo, rhs)
    write_message(msg_ref, packed, field, near_ref[...], rhs)


def second_kernel(tail_ref, *refs):
    levels = len(refs) - 10
    parts = refs[:levels]
    b_ref, near_ref, dhi_ref, dlo_ref, qhi_ref, qlo_ref = refs[levels:levels + 6]
    r_ref, image_ref, next_ref, msg_ref = refs[levels + 6:]
    rhs = b_ref.shape[0]
    half = qhi_ref.shape[0] // levels // 2
    norm = to_column(tail_ref[0:1], rhs)
    product = to_column(tail_ref[1:2], rhs)
    alpha = norm / product
    far = far_product([part[:half] for part in parts], qhi_ref[...], qlo_ref[...], rhs)
    image = near_ref[...] + far
    image_ref[...] = image
    field = b_ref[...] - alpha * image
    r_ref[...] = field
    field_hi, field_lo = split2(field)
    both = jnp.concatenate([field_hi, field_lo], axis=0)
    packed = pack_projection(qhi_ref[...], qlo_ref[...], both, rhs)
    near = near_product(both, field_hi, dhi_ref[...], dlo_ref[...], rhs)
    next_ref[...] = near
    write_message(msg_ref, packed, field, near, rhs)


def third_kernel(order_ref, old_ref, tail_ref, *refs):
    levels = len(refs) - 8
    parts = refs[:levels]
    b_ref, image_ref, r_ref, near_ref, qhi_ref, qlo_ref, x_out, r_out = refs[levels:]
    rhs, leaf = b_ref.shape
    half = qhi_ref.shape[0] // levels // 2
    norm_old = to_column(old_ref[0:1], rhs)
    alpha_old = norm_old / to_column(old_ref[1:2], rhs)
    norm = to_column(tail_ref[0:1], rhs)
    product = to_column(tail_ref[1:2], rhs)
    ratio = norm / norm_old
    alpha = norm / (product - ratio * norm / alpha_old)
    far = far_product([part[:half] for part in parts], qhi_ref[...], qlo_ref[...], rhs)
    direction = r_ref[...] + ratio * b_ref[...]
    along = near_ref[...] + far + ratio * image_ref[...]
    x = alpha_old * b_ref[...] + alpha * direction
    r = r_ref[...] - alpha * along
    three = jnp.concatenate(split3(x) + split3(r), axis=0)
    chunk = 256
    for n in range(leaf // chunk):
        cols = pl.ds(n * chunk, chunk)
        index = lax.broadcasted_iota(jnp.int32, (chunk, leaf), 0) + n * chunk
        onehot = jnp.where(index == order_ref[...], 1.0, 0.0).astype(BF16)
        got = dot_nt(three, onehot)
        x_out[:, cols] = got[:rhs] + got[rhs:2 * rhs] + got[2 * rhs:3 * rhs]
        r_out[:, cols] = got[3 * rhs:4 * rhs] + got[4 * rhs:5 * rhs] + got[5 * rhs:]


def swapped(value, level):
    mask = 2**level + (1 if level else 0)
    count = lax.axis_size("wide") * lax.axis_size("narrow")
    return lax.ppermute(value, AXES, [(source, source ^ mask) for source in range(count)])


def butterfly(message, levels, half):
    parts = []
    for level in range(levels):
        other = swapped(message, level)
        parts.append(other)
        cross = 2.0 * jnp.sum(message[:half] * other[:half], axis=0, keepdims=True)
        merged = message[half:] + other[half:]
        message = merged + jnp.pad(cross, ((merged.shape[0] - TAIL + 1, TAIL - 2), (0, 0)))
    return parts, message


def local(right_side, leaf_blocks, factors, leaf_order):
    leaf = leaf_blocks.shape[1]
    levels, rank, _ = factors.shape
    rhs = right_side.shape[0]
    half = rank // 2
    order = lax.rem(leaf_order, leaf).reshape(1, leaf)
    field = jax.ShapeDtypeStruct((rhs, leaf), F32)
    message = jax.ShapeDtypeStruct((levels * half + TAIL, 2 * rhs), F32)
    matrix = jax.ShapeDtypeStruct((leaf, leaf), BF16)
    basis = jax.ShapeDtypeStruct((levels * rank, leaf), BF16)
    params = pltpu.CompilerParams(vmem_limit_bytes=32 * 1024 * 1024)
    chunks = leaf // 256
    b, near, msg, dhi, dlo, qhi, qlo = pl.pallas_call(
        first_kernel,
        out_shape=(field, field, message, matrix, matrix, basis, basis),
        in_specs=[VMEM, VMEM, HBM, HBM],
        out_specs=(VMEM,) * 7,
        scratch_shapes=[
            pltpu.VMEM((leaf, leaf), F32),
            pltpu.VMEM(factors.shape, F32),
            pltpu.SemaphoreType.DMA((chunks + 1,)),
        ],
        compiler_params=params,
        name="first",
    )(order, right_side, leaf_blocks, factors)
    parts, tail = butterfly(msg, levels, half)
    r, image, near_next, msg = pl.pallas_call(
        second_kernel,
        out_shape=(field, field, field, message),
        in_specs=[VMEM] * (7 + levels),
        out_specs=(VMEM,) * 4,
        compiler_params=params,
        name="second",
    )(tail, *parts, b, near, dhi, dlo, qhi, qlo)
    parts, tail_next = butterfly(msg, levels, half)
    return pl.pallas_call(
        third_kernel,
        out_shape=(field, field),
        in_specs=[VMEM] * (9 + levels),
        out_specs=(VMEM,) * 2,
        compiler_params=params,
        name="third",
    )(order, tail, tail_next, *parts, b, image, r, near_next, qhi, qlo)


def solution(mesh):
    placed = (
        P(None, AXES),
        P(AXES, None),
        P(None, None, AXES),
        P(AXES),
    )
    return jax.shard_map(
        local,
        mesh=mesh,
        in_specs=placed,
        out_specs=(P(None, AXES), P(None, AXES)),
        check_vma=False,
    )
```

```python
import jax
import jax.numpy as jnp
from jax import lax
from jax.experimental import pallas as pl
from jax.experimental.pallas import tpu as pltpu
from jax.sharding import PartitionSpec as P

AXES = ("wide", "narrow")
F32 = jnp.float32
BF16 = jnp.bfloat16
TAIL = 8
VMEM = pl.BlockSpec(memory_space=pltpu.VMEM)
HBM = pl.BlockSpec(memory_space=pltpu.HBM)


def dot(a, b):
    return jnp.dot(a, b, preferred_element_type=F32)


def dot_nt(a, b):
    return lax.dot_general(a, b, (((1,), (1,)), ((), ())), preferred_element_type=F32)


def split2(value):
    high = value.astype(BF16)
    return high, (value - high.astype(F32)).astype(BF16)


def split3(value):
    high = value.astype(BF16)
    rest = value - high.astype(F32)
    mid = rest.astype(BF16)
    return high, mid, (rest - mid.astype(F32)).astype(BF16)


def eye_mask(rows, lanes, period):
    row = lax.broadcasted_iota(jnp.int32, (rows, lanes), 0)
    lane = lax.broadcasted_iota(jnp.int32, (rows, lanes), 1)
    return (lane == row) | (lane == row + period)


def to_row(column, lanes):
    rows = column.shape[0]
    row = lax.broadcasted_iota(jnp.int32, (rows, lanes), 0)
    lane = lax.broadcasted_iota(jnp.int32, (rows, lanes), 1)
    return jnp.sum(jnp.where(row == lane, column, 0.0), axis=0, keepdims=True)


def to_column(row, rows):
    lanes = row.shape[1]
    return jnp.sum(jnp.where(eye_mask(rows, lanes, rows), row, 0.0), axis=1, keepdims=True)


def pack_projection(q_hi, q_lo, both, rhs):
    result = dot_nt(q_hi, both) + dot_nt(q_lo, both)
    full = result + pltpu.roll(result, rhs, 1)
    half = full.shape[0] // 2
    lane = lax.broadcasted_iota(jnp.int32, (half, full.shape[1]), 1)
    return jnp.where(lane < rhs, full[:half], full[half:])


def write_message(msg_ref, packed, field, near, rhs):
    lanes = 2 * rhs
    square = jnp.sum(field * field, axis=1, keepdims=True)
    product = jnp.sum(field * near, axis=1, keepdims=True)
    rows = packed.shape[0]
    msg_ref[:rows] = packed
    index = lax.broadcasted_iota(jnp.int32, (TAIL, lanes), 0)
    tail = jnp.where(index == 0, to_row(square, lanes), jnp.where(index == 1, to_row(product, lanes), 0.0))
    msg_ref[rows:] = tail


def near_product(both, field_hi, d_hi, d_lo, rhs):
    wide = dot(both, d_hi)
    return wide[:rhs] + wide[rhs:] + dot(field_hi, d_lo)


def far_product(parts, q_hi, q_lo, rhs):
    stacked = jnp.concatenate(parts, axis=0)
    turned = stacked.T
    half = q_hi.shape[0] // 2
    total = None
    for side in range(2):
        hi, lo = split2(turned[side * rhs:(side + 1) * rhs])
        both = jnp.concatenate([hi, lo], axis=0)
        wide = dot(both, q_hi[side * half:(side + 1) * half])
        part = wide[:rhs] + wide[rhs:] + dot(hi, q_lo[side * half:(side + 1) * half])
        total = part if total is None else total + part
    return total


def first_kernel(order_hbm, rs_hbm, d_hbm, f_hbm, b_ref, near_ref, msg_ref, dhi_ref, dlo_ref, qhi_ref, qlo_ref, order_ref,
                 rs_ref, d_ref, f_ref, sems):
    levels, rank, leaf = f_ref.shape
    rhs = rs_ref.shape[0]
    half = rank // 2
    chunk = 256
    chunks = leaf // chunk
    order_copy = pltpu.make_async_copy(order_hbm, order_ref, sems.at[chunks + 1])
    order_copy.start()
    rs_copy = pltpu.make_async_copy(rs_hbm, rs_ref, sems.at[chunks + 2])
    rs_copy.start()
    f_copy = pltpu.make_async_copy(f_hbm, f_ref, sems.at[chunks])
    f_copy.start()
    d_copies = []
    for n in range(chunks):
        cols = pl.ds(n * chunk, chunk)
        copy = pltpu.make_async_copy(d_hbm.at[:, cols], d_ref.at[:, cols], sems.at[n])
        copy.start()
        d_copies.append(copy)
    order_copy.wait()
    rs_copy.wait()
    hi, mid, lo = split3(rs_ref[...])
    three = jnp.concatenate([hi, mid, lo], axis=0)
    for n in range(chunks):
        cols = pl.ds(n * chunk, chunk)
        index = lax.broadcasted_iota(jnp.int32, (leaf, chunk), 0)
        local_order = lax.rem(order_ref[:, cols], leaf)
        onehot = jnp.where(index == local_order, 1.0, 0.0).astype(BF16)
        got = dot(three, onehot)
        b_ref[:, cols] = got[:rhs] + got[rhs:2 * rhs] + got[2 * rhs:]
    field = b_ref[...]
    field_hi, field_lo = split2(field)
    both = jnp.concatenate([field_hi, field_lo], axis=0)
    f_copy.wait()
    for level in range(levels):
        for side in range(2):
            hi, lo = split2(f_ref[level, pl.ds(side * half, half)])
            rows = pl.ds((side * levels + level) * half, half)
            qhi_ref[rows] = hi
            qlo_ref[rows] = lo
    packed = pack_projection(qhi_ref[...], qlo_ref[...], both, rhs)
    for n in range(chunks):
        cols = pl.ds(n * chunk, chunk)
        d_copies[n].wait()
        d_hi, d_lo = split2(d_ref[:, cols])
        dhi_ref[:, cols] = d_hi
        dlo_ref[:, cols] = d_lo
        near_ref[:, cols] = near_product(both, field_hi, d_hi, d_lo, rhs)
    write_message(msg_ref, packed, field, near_ref[...], rhs)


def second_kernel(tail_ref, *refs):
    levels = len(refs) - 10
    parts = refs[:levels]
    b_ref, near_ref, dhi_ref, dlo_ref, qhi_ref, qlo_ref = refs[levels:levels + 6]
    r_ref, image_ref, next_ref, msg_ref = refs[levels + 6:]
    rhs = b_ref.shape[0]
    half = qhi_ref.shape[0] // levels // 2
    norm = to_column(tail_ref[0:1], rhs)
    product = to_column(tail_ref[1:2], rhs)
    alpha = norm / product
    far = far_product([part[:half] for part in parts], qhi_ref[...], qlo_ref[...], rhs)
    image = near_ref[...] + far
    image_ref[...] = image
    field = b_ref[...] - alpha * image
    r_ref[...] = field
    field_hi, field_lo = split2(field)
    both = jnp.concatenate([field_hi, field_lo], axis=0)
    packed = pack_projection(qhi_ref[...], qlo_ref[...], both, rhs)
    near = near_product(both, field_hi, dhi_ref[...], dlo_ref[...], rhs)
    next_ref[...] = near
    write_message(msg_ref, packed, field, near, rhs)


def third_kernel(order_ref, old_ref, tail_ref, *refs):
    levels = len(refs) - 8
    parts = refs[:levels]
    b_ref, image_ref, r_ref, near_ref, qhi_ref, qlo_ref, x_out, r_out = refs[levels:]
    rhs, leaf = b_ref.shape
    half = qhi_ref.shape[0] // levels // 2
    norm_old = to_column(old_ref[0:1], rhs)
    alpha_old = norm_old / to_column(old_ref[1:2], rhs)
    norm = to_column(tail_ref[0:1], rhs)
    product = to_column(tail_ref[1:2], rhs)
    ratio = norm / norm_old
    alpha = norm / (product - ratio * norm / alpha_old)
    far = far_product([part[:half] for part in parts], qhi_ref[...], qlo_ref[...], rhs)
    direction = r_ref[...] + ratio * b_ref[...]
    along = near_ref[...] + far + ratio * image_ref[...]
    x = alpha_old * b_ref[...] + alpha * direction
    r = r_ref[...] - alpha * along
    three = jnp.concatenate(split3(x) + split3(r), axis=0)
    chunk = 256
    local_order = lax.rem(order_ref[...], leaf)
    for n in range(leaf // chunk):
        cols = pl.ds(n * chunk, chunk)
        index = lax.broadcasted_iota(jnp.int32, (chunk, leaf), 0) + n * chunk
        onehot = jnp.where(index == local_order, 1.0, 0.0).astype(BF16)
        got = dot_nt(three, onehot)
        x_out[:, cols] = got[:rhs] + got[rhs:2 * rhs] + got[2 * rhs:3 * rhs]
        r_out[:, cols] = got[3 * rhs:4 * rhs] + got[4 * rhs:5 * rhs] + got[5 * rhs:]


def swapped(value, level):
    mask = 2**level + (1 if level else 0)
    count = lax.axis_size("wide") * lax.axis_size("narrow")
    return lax.ppermute(value, AXES, [(source, source ^ mask) for source in range(count)])


def butterfly(message, levels, half):
    parts = []
    for level in range(levels):
        other = swapped(message, level)
        parts.append(other)
        cross = 2.0 * jnp.sum(message[:half] * other[:half], axis=0, keepdims=True)
        merged = message[half:] + other[half:]
        message = merged + jnp.pad(cross, ((merged.shape[0] - TAIL + 1, TAIL - 2), (0, 0)))
    return parts, message


def local(right_side, leaf_blocks, factors, leaf_order):
    leaf = leaf_blocks.shape[1]
    levels, rank, _ = factors.shape
    rhs = right_side.shape[0]
    half = rank // 2
    order = leaf_order.reshape(1, leaf)
    hbm = [pltpu.with_memory_space_constraint(value, pltpu.HBM) for value in (order, right_side, leaf_blocks, factors)]
    field = jax.ShapeDtypeStruct((rhs, leaf), F32)
    message = jax.ShapeDtypeStruct((levels * half + TAIL, 2 * rhs), F32)
    matrix = jax.ShapeDtypeStruct((leaf, leaf), BF16)
    basis = jax.ShapeDtypeStruct((levels * rank, leaf), BF16)
    params = pltpu.CompilerParams(vmem_limit_bytes=32 * 1024 * 1024)
    chunks = leaf // 256
    b, near, msg, dhi, dlo, qhi, qlo, order = pl.pallas_call(
        first_kernel,
        out_shape=(field, field, message, matrix, matrix, basis, basis, jax.ShapeDtypeStruct((1, leaf), jnp.int32)),
        in_specs=[HBM] * 4,
        out_specs=(VMEM,) * 8,
        scratch_shapes=[
            pltpu.VMEM((rhs, leaf), F32),
            pltpu.VMEM((leaf, leaf), F32),
            pltpu.VMEM(factors.shape, F32),
            pltpu.SemaphoreType.DMA((chunks + 3,)),
        ],
        compiler_params=params,
        name="first",
    )(*hbm)
    parts, tail = butterfly(msg, levels, half)
    r, image, near_next, msg = pl.pallas_call(
        second_kernel,
        out_shape=(field, field, field, message),
        in_specs=[VMEM] * (7 + levels),
        out_specs=(VMEM,) * 4,
        compiler_params=params,
        name="second",
    )(tail, *parts, b, near, dhi, dlo, qhi, qlo)
    parts, tail_next = butterfly(msg, levels, half)
    return pl.pallas_call(
        third_kernel,
        out_shape=(field, field),
        in_specs=[VMEM] * (9 + levels),
        out_specs=(VMEM,) * 2,
        compiler_params=params,
        name="third",
    )(order, tail, tail_next, *parts, b, image, r, near_next, qhi, qlo)


def solution(mesh):
    placed = (
        P(None, AXES),
        P(AXES, None),
        P(None, None, AXES),
        P(AXES),
    )
    return jax.shard_map(
        local,
        mesh=mesh,
        in_specs=placed,
        out_specs=(P(None, AXES), P(None, AXES)),
        check_vma=False,
    )
```

```python
import jax
import jax.numpy as jnp
from jax import lax
from jax.experimental import pallas as pl
from jax.experimental.pallas import tpu as pltpu
from jax.sharding import PartitionSpec as P

AXES = ("wide", "narrow")
F32 = jnp.float32
BF16 = jnp.bfloat16
TAIL = 8
FLOPS = 2 * 10**9
VMEM = pl.BlockSpec(memory_space=pltpu.VMEM)
HBM = pl.BlockSpec(memory_space=pltpu.HBM)


def dot(a, b):
    return jnp.dot(a, b, preferred_element_type=F32)


def dot_nt(a, b):
    return lax.dot_general(a, b, (((1,), (1,)), ((), ())), preferred_element_type=F32)


def split2(value):
    high = value.astype(BF16)
    return high, (value - high.astype(F32)).astype(BF16)


def iota(shape, axis):
    return lax.broadcasted_iota(jnp.int32, shape, axis)


def to_row(column, lanes):
    shape = (column.shape[0], lanes)
    return jnp.sum(jnp.where(iota(shape, 0) == iota(shape, 1), column, 0.0), axis=0, keepdims=True)


def to_column(row, rows):
    shape = (rows, row.shape[1])
    return jnp.sum(jnp.where(iota(shape, 0) == lax.rem(iota(shape, 1), rows), row, 0.0), axis=1, keepdims=True)


def own_side():
    index = lax.axis_index("wide") * lax.axis_size("narrow") + lax.axis_index("narrow")
    side = index & 1
    for bit in range(1, (lax.axis_size("wide") * lax.axis_size("narrow")).bit_length() - 1):
        side = side ^ ((index >> bit) & 1)
    return side


def write_projection(msg_ref, own_ref, q_hi, q_lo, both, levels, rhs):
    quarter = rhs // 2
    full = dot_nt(q_hi, both) + dot_nt(q_lo, both)
    full = full + pltpu.roll(full, rhs, 1)
    rows = own_ref.shape[0]
    blocks = [full[group * rows:(group + 1) * rows] for group in range(4)]
    group = iota((rows, 2 * rhs), 1) // quarter
    lower = jnp.where((group & 1) == 0, jnp.where(group < 2, blocks[0], blocks[2]),
                      jnp.where(group < 2, pltpu.roll(blocks[1], quarter, 1), pltpu.roll(blocks[3], quarter, 1)))
    back = 2 * rhs - quarter
    upper = jnp.where((group & 1) == 1, jnp.where(group < 2, blocks[1], blocks[3]),
                      jnp.where(group < 2, pltpu.roll(blocks[0], back, 1), pltpu.roll(blocks[2], back, 1)))
    first = full[4 * rows:]
    half = first.shape[0] // 2
    msg_ref[:half] = jnp.where(iota((half, 2 * rhs), 1) < rhs, first[:half], first[half:])
    even = own_side() == 0
    own_ref[...] = jnp.where(even, lower, upper)
    msg_ref[half:] = jnp.where(even, upper, lower)


def near_product(both, field_hi, d_hi, d_lo, rhs):
    wide = dot(both, d_hi)
    return wide[:rhs] + wide[rhs:] + dot(field_hi, d_lo)


def write_tail(tail_ref, field, near):
    shape = tail_ref.shape
    square = to_row(jnp.sum(field * field, axis=1, keepdims=True), shape[1])
    product = to_row(jnp.sum(field * near, axis=1, keepdims=True), shape[1])
    index = iota(shape, 0)
    tail_ref[...] = jnp.where(index == 0, square, jnp.where(index == 1, product, 0.0))


def far_product(zero_ref, own_ref, other_ref, q_hi, q_lo, rhs):
    lanes = 2 * rhs
    quarter = rhs // 2
    rows = own_ref.shape[0] - TAIL
    even = own_side() == 0
    own, other = own_ref[:rows], other_ref[:rows]
    lower, upper = jnp.where(even, own, other), jnp.where(even, other, own)
    lane = iota((rows, lanes), 1)
    pieces = []
    for group in range(4):
        left = pltpu.roll(lower, (lanes - group * quarter) % lanes, 1) if group else lower
        right = pltpu.roll(upper, (lanes + quarter - group * quarter) % lanes, 1) if group != 1 else upper
        pieces.append(jnp.where(lane < quarter, left, right))
    zero = zero_ref[:own_half(q_hi, rows)]
    pieces += [zero, pltpu.roll(zero, rhs, 1)]
    turned = jnp.concatenate(pieces, axis=0).T[:rhs]
    hi, lo = split2(turned)
    wide = dot(jnp.concatenate([hi, lo], axis=0), q_hi)
    return wide[:rhs] + wide[rhs:] + dot(hi, q_lo)


def own_half(q_hi, rows):
    return (q_hi.shape[0] - 4 * rows) // 2


def scalars(own_ref, other_ref, rhs):
    rows = own_ref.shape[0] - TAIL
    own, other = own_ref[rows:], other_ref[rows:]
    both = own + other
    norm = to_column(both[0:1], rhs)
    product = to_column(both[1:2], rhs)
    quarter = rhs // 2
    shape = (rhs, own.shape[1])
    row = iota(shape, 0)
    mine = (row // quarter) == own_side()
    cross = jnp.where(mine, own[2:3], other[2:3])
    cross = jnp.where(lax.rem(iota(shape, 1), quarter) == lax.rem(row, quarter), cross, 0.0)
    return norm, product + jnp.sum(cross, axis=1, keepdims=True)


def start_kernel(order_hbm, rs_hbm, f_hbm, b_ref, msg_ref, own_ref, qhi_ref, qlo_ref, order_ref, rs_ref, f_ref, sems):
    levels, rank, leaf = f_ref.shape
    rhs = rs_ref.shape[0]
    chunk = 256
    copies = [
        pltpu.make_async_copy(order_hbm, order_ref, sems.at[0]),
        pltpu.make_async_copy(rs_hbm, rs_ref, sems.at[1]),
        pltpu.make_async_copy(f_hbm, f_ref, sems.at[2]),
    ]
    for copy in copies:
        copy.start()
    for copy in copies:
        copy.wait()
    two = jnp.concatenate(split2(rs_ref[...]), axis=0)
    local_order = lax.rem(order_ref[...], leaf)
    for n in range(leaf // chunk):
        cols = pl.ds(n * chunk, chunk)
        onehot = jnp.where(iota((leaf, chunk), 0) == local_order[:, n * chunk:(n + 1) * chunk], 1.0, 0.0).astype(BF16)
        got = dot(two, onehot)
        b_ref[:, cols] = got[:rhs] + got[rhs:]
    block = rank // 4
    for level in range(levels):
        for group in range(4):
            hi, lo = split2(f_ref[level, pl.ds(group * block, block)])
            if level:
                rows = pl.ds((group * (levels - 1) + level - 1) * block, block)
            else:
                rows = pl.ds((4 * (levels - 1) + group) * block, block)
            qhi_ref[rows] = hi
            qlo_ref[rows] = lo
    both = jnp.concatenate(split2(b_ref[...]), axis=0)
    write_projection(msg_ref, own_ref, qhi_ref[...], qlo_ref[...], both, levels, rhs)


def near_kernel(b_ref, d_ref, near_ref, tail_ref, dhi_ref, dlo_ref):
    rhs, leaf = b_ref.shape
    chunk = 256
    field = b_ref[...]
    field_hi, field_lo = split2(field)
    both = jnp.concatenate([field_hi, field_lo], axis=0)
    for n in range(leaf // chunk):
        cols = pl.ds(n * chunk, chunk)
        d_hi, d_lo = split2(d_ref[:, cols])
        dhi_ref[:, cols] = d_hi
        dlo_ref[:, cols] = d_lo
        near_ref[:, cols] = near_product(both, field_hi, dhi_ref[:, cols], dlo_ref[:, cols], rhs)
    write_tail(tail_ref, field, near_ref[...])


def step_kernel(zero_ref, own_ref, other_ref, b_ref, near_ref, qhi_ref, qlo_ref, r_ref, image_ref, msg_ref, mine_ref):
    rhs = b_ref.shape[0]
    levels = mine_ref.shape[0] // (qhi_ref.shape[0] // 4 - mine_ref.shape[0]) + 1
    norm, product = scalars(own_ref, other_ref, rhs)
    alpha = norm / product
    far = far_product(zero_ref, own_ref, other_ref, qhi_ref[...], qlo_ref[...], rhs)
    image = near_ref[...] + far
    image_ref[...] = image
    field = b_ref[...] - alpha * image
    r_ref[...] = field
    both = jnp.concatenate(split2(field), axis=0)
    write_projection(msg_ref, mine_ref, qhi_ref[...], qlo_ref[...], both, levels, rhs)


def again_kernel(r_ref, dhi_ref, dlo_ref, near_ref, tail_ref):
    rhs = r_ref.shape[0]
    field = r_ref[...]
    field_hi, field_lo = split2(field)
    both = jnp.concatenate([field_hi, field_lo], axis=0)
    near = near_product(both, field_hi, dhi_ref[...], dlo_ref[...], rhs)
    near_ref[...] = near
    write_tail(tail_ref, field, near)


def last_kernel(order_ref, zero_ref, own_ref, other_ref, old_own_ref, old_other_ref, b_ref, image_ref, r_ref, near_ref,
                qhi_ref, qlo_ref, x_out, r_out):
    rhs, leaf = b_ref.shape
    norm_old, product_old = scalars(old_own_ref, old_other_ref, rhs)
    alpha_old = norm_old / product_old
    norm, product = scalars(own_ref, other_ref, rhs)
    ratio = norm / norm_old
    alpha = norm / (product - ratio * norm / alpha_old)
    far = far_product(zero_ref, own_ref, other_ref, qhi_ref[...], qlo_ref[...], rhs)
    direction = r_ref[...] + ratio * b_ref[...]
    along = near_ref[...] + far + ratio * image_ref[...]
    x = alpha_old * b_ref[...] + alpha * direction
    r = r_ref[...] - alpha * along
    four = jnp.concatenate(split2(x) + split2(r), axis=0)
    chunk = 256
    local_order = lax.rem(order_ref[...], leaf)
    for n in range(leaf // chunk):
        cols = pl.ds(n * chunk, chunk)
        index = iota((chunk, leaf), 0) + n * chunk
        onehot = jnp.where(index == local_order, 1.0, 0.0).astype(BF16)
        got = dot_nt(four, onehot)
        x_out[:, cols] = got[:rhs] + got[rhs:2 * rhs]
        r_out[:, cols] = got[2 * rhs:3 * rhs] + got[3 * rhs:]


def swapped(value, mask):
    mask = mask ^ (mask.bit_count() & 1 if mask > 1 else 0)
    count = lax.axis_size("wide") * lax.axis_size("narrow")
    return lax.ppermute(value, AXES, [(source, source ^ mask) for source in range(count)])


def column_products(left, right):
    return jnp.sum(left * right, axis=0, keepdims=True)


def with_row(merged, row, place):
    return merged + jnp.pad(row, ((merged.shape[0] - TAIL + place, TAIL - place - 1), (0, 0)))


def butterfly(first, own, tail_of, levels, rank):
    half, part = rank // 2, rank // 4
    got = swapped(first, 1)
    tail = with_row(tail_of(), column_products(first[:half], got[:half]), 1)
    message = jnp.concatenate([own + got[half:], tail])
    parts = []
    level = 1
    low = lax.axis_size("narrow").bit_length() - 1
    while level < levels:
        if level < low or level + 1 == levels:
            other = swapped(message, 2**level)
            parts.append(other[:part])
            cross = 2.0 * column_products(message[:part], other[:part])
            message = with_row(message[part:] + other[part:], cross, 2)
            level += 1
        else:
            x = swapped(message, 2**level)
            y = swapped(message, 2 * 2**level)
            z = swapped(message, 3 * 2**level)
            far = y + z
            pair = message[part:] + x[part:]
            parts += [x[:part], far[part:2 * part]]
            cross = column_products(message[:part], x[:part]) + column_products(y[:part], z[:part])
            cross = 2.0 * (cross + column_products(pair[:part], far[part:2 * part]))
            message = with_row(pair[part:] + far[2 * part:], cross, 2)
            level += 2
    mine = jnp.concatenate(parts + [message])
    return got, mine, swapped(mine, 1)


def call(kernel, name, outs, in_specs, scratch=(), flops=0):
    return pl.pallas_call(
        kernel,
        out_shape=outs,
        in_specs=in_specs,
        out_specs=tuple(VMEM for _ in outs),
        scratch_shapes=list(scratch),
        compiler_params=pltpu.CompilerParams(vmem_limit_bytes=32 * 1024 * 1024),
        cost_estimate=pl.CostEstimate(flops=flops, bytes_accessed=0, transcendentals=0) if flops else None,
        name=name,
    )


def local(right_side, leaf_blocks, factors, leaf_order):
    leaf = leaf_blocks.shape[1]
    levels, rank, _ = factors.shape
    rhs = right_side.shape[0]
    lanes = 2 * rhs
    rows = (levels - 1) * rank // 4
    pinned = [pltpu.with_memory_space_constraint(value, pltpu.HBM) for value in (leaf_order.reshape(1, leaf), right_side, factors)]
    field = jax.ShapeDtypeStruct((rhs, leaf), F32)
    message = jax.ShapeDtypeStruct((rank // 2 + rows, lanes), F32)
    own = jax.ShapeDtypeStruct((rows, lanes), F32)
    tail = jax.ShapeDtypeStruct((TAIL, lanes), F32)
    matrix = jax.ShapeDtypeStruct((leaf, leaf), BF16)
    basis = jax.ShapeDtypeStruct((levels * rank, leaf), BF16)
    scratch = [pltpu.VMEM(right_side.shape, F32), pltpu.VMEM(factors.shape, F32), pltpu.SemaphoreType.DMA((3,))]
    b, first, mine, qhi, qlo, order = call(
        start_kernel, "start", (field, message, own, basis, basis, jax.ShapeDtypeStruct((1, leaf), jnp.int32)),
        [HBM] * 3, scratch)(*pinned)
    kept = {}

    def first_tail():
        kept["near"], value, kept["dhi"], kept["dlo"] = call(
            near_kernel, "near", (field, tail, matrix, matrix), [VMEM] * 2, flops=FLOPS)(b, leaf_blocks)
        return value

    zero, ours, theirs = butterfly(first, mine, first_tail, levels, rank)
    r, image, first, mine = call(step_kernel, "step", (field, field, message, own), [VMEM] * 7)(
        zero, ours, theirs, b, kept["near"], qhi, qlo)

    def next_tail():
        kept["next"], value = call(again_kernel, "again", (field, tail), [VMEM] * 3, flops=FLOPS)(r, kept["dhi"], kept["dlo"])
        return value

    zero, ours_next, theirs_next = butterfly(first, mine, next_tail, levels, rank)
    return call(last_kernel, "last", (field, field), [VMEM] * 12)(
        order, zero, ours_next, theirs_next, ours, theirs, b, image, r, kept["next"], qhi, qlo)


def solution(mesh):
    placed = (
        P(None, AXES),
        P(AXES, None),
        P(None, None, AXES),
        P(AXES),
    )
    return jax.shard_map(
        local,
        mesh=mesh,
        in_specs=placed,
        out_specs=(P(None, AXES), P(None, AXES)),
        check_vma=False,
    )
```

```python
import jax
import jax.numpy as jnp
from jax import lax
from jax.experimental import pallas as pl
from jax.experimental.pallas import tpu as pltpu
from jax.sharding import PartitionSpec as P

AXES = ("wide", "narrow")
F32 = jnp.float32
BF16 = jnp.bfloat16
TAIL = 8
FLOPS = 2 * 10**9
VMEM = pl.BlockSpec(memory_space=pltpu.VMEM)
HBM = pl.BlockSpec(memory_space=pltpu.HBM)


def dot(a, b):
    return jnp.dot(a, b, preferred_element_type=F32)


def dot_nt(a, b):
    return lax.dot_general(a, b, (((1,), (1,)), ((), ())), preferred_element_type=F32)


def split2(value):
    high = value.astype(BF16)
    return high, (value - high.astype(F32)).astype(BF16)


def iota(shape, axis):
    return lax.broadcasted_iota(jnp.int32, shape, axis)


def to_row(column, lanes):
    shape = (column.shape[0], lanes)
    return jnp.sum(jnp.where(iota(shape, 0) == iota(shape, 1), column, 0.0), axis=0, keepdims=True)


def to_column(row, rows):
    shape = (rows, row.shape[1])
    return jnp.sum(jnp.where(iota(shape, 0) == lax.rem(iota(shape, 1), rows), row, 0.0), axis=1, keepdims=True)


def own_side():
    index = lax.axis_index("wide") * lax.axis_size("narrow") + lax.axis_index("narrow")
    side = index & 1
    for bit in range(1, (lax.axis_size("wide") * lax.axis_size("narrow")).bit_length() - 1):
        side = side ^ ((index >> bit) & 1)
    return side


def write_projection(msg_ref, own_ref, q_hi, q_lo, both, levels, rhs):
    quarter = rhs // 2
    full = dot_nt(q_hi, both) + dot_nt(q_lo, both)
    full = full + pltpu.roll(full, rhs, 1)
    rows = own_ref.shape[0]
    blocks = [full[group * rows:(group + 1) * rows] for group in range(4)]
    group = iota((rows, 2 * rhs), 1) // quarter
    lower = jnp.where((group & 1) == 0, jnp.where(group < 2, blocks[0], blocks[2]),
                      jnp.where(group < 2, pltpu.roll(blocks[1], quarter, 1), pltpu.roll(blocks[3], quarter, 1)))
    back = 2 * rhs - quarter
    upper = jnp.where((group & 1) == 1, jnp.where(group < 2, blocks[1], blocks[3]),
                      jnp.where(group < 2, pltpu.roll(blocks[0], back, 1), pltpu.roll(blocks[2], back, 1)))
    first = full[4 * rows:]
    half = first.shape[0] // 2
    msg_ref[:half] = jnp.where(iota((half, 2 * rhs), 1) < rhs, first[:half], first[half:])
    even = own_side() == 0
    own_ref[...] = jnp.where(even, lower, upper)
    msg_ref[half:] = jnp.where(even, upper, lower)


def near_product(both, field_hi, d_hi, d_lo, rhs):
    wide = dot(both, d_hi)
    return wide[:rhs] + wide[rhs:] + dot(field_hi, d_lo)


def write_tail(tail_ref, field, near):
    shape = tail_ref.shape
    square = to_row(jnp.sum(field * field, axis=1, keepdims=True), shape[1])
    product = to_row(jnp.sum(field * near, axis=1, keepdims=True), shape[1])
    index = iota(shape, 0)
    tail_ref[...] = jnp.where(index == 0, square, jnp.where(index == 1, product, 0.0))


def far_product(zero_ref, own_ref, other_ref, q_hi, q_lo, rhs):
    lanes = 2 * rhs
    quarter = rhs // 2
    rows = own_ref.shape[0] - TAIL
    even = own_side() == 0
    own, other = own_ref[:rows], other_ref[:rows]
    lower, upper = jnp.where(even, own, other), jnp.where(even, other, own)
    lane = iota((rows, lanes), 1)
    pieces = []
    for group in range(4):
        left = pltpu.roll(lower, (lanes - group * quarter) % lanes, 1) if group else lower
        right = pltpu.roll(upper, (lanes + quarter - group * quarter) % lanes, 1) if group != 1 else upper
        pieces.append(jnp.where(lane < quarter, left, right))
    zero = zero_ref[:own_half(q_hi, rows)]
    pieces += [zero, pltpu.roll(zero, rhs, 1)]
    turned = jnp.concatenate(pieces, axis=0).T[:rhs]
    hi, lo = split2(turned)
    wide = dot(jnp.concatenate([hi, lo], axis=0), q_hi)
    return wide[:rhs] + wide[rhs:] + dot(hi, q_lo)


def own_half(q_hi, rows):
    return (q_hi.shape[0] - 4 * rows) // 2


def scalars(own_ref, other_ref, rhs):
    rows = own_ref.shape[0] - TAIL
    own, other = own_ref[rows:], other_ref[rows:]
    both = own + other
    norm = to_column(both[0:1], rhs)
    product = to_column(both[1:2], rhs)
    quarter = rhs // 2
    shape = (rhs, own.shape[1])
    row = iota(shape, 0)
    mine = (row // quarter) == own_side()
    cross = jnp.where(mine, own[2:3], other[2:3])
    cross = jnp.where(lax.rem(iota(shape, 1), quarter) == lax.rem(row, quarter), cross, 0.0)
    return norm, product + jnp.sum(cross, axis=1, keepdims=True)


def start_kernel(order_hbm, rs_hbm, f_hbm, b_ref, msg_ref, own_ref, qhi_ref, qlo_ref, order_ref, rs_ref, f_ref, sems):
    levels, rank, leaf = f_ref.shape
    rhs = rs_ref.shape[0]
    chunk = 256
    copies = [
        pltpu.make_async_copy(order_hbm, order_ref, sems.at[0]),
        pltpu.make_async_copy(rs_hbm, rs_ref, sems.at[1]),
        pltpu.make_async_copy(f_hbm, f_ref, sems.at[2]),
    ]
    for copy in copies:
        copy.start()
    for copy in copies:
        copy.wait()
    two = jnp.concatenate(split2(rs_ref[...]), axis=0)
    local_order = lax.rem(order_ref[...], leaf)
    for n in range(leaf // chunk):
        cols = pl.ds(n * chunk, chunk)
        onehot = jnp.where(iota((leaf, chunk), 0) == local_order[:, n * chunk:(n + 1) * chunk], 1.0, 0.0).astype(BF16)
        got = dot(two, onehot)
        b_ref[:, cols] = got[:rhs] + got[rhs:]
    block = rank // 4
    for level in range(levels):
        for group in range(4):
            hi, lo = split2(f_ref[level, pl.ds(group * block, block)])
            if level:
                rows = pl.ds((group * (levels - 1) + level - 1) * block, block)
            else:
                rows = pl.ds((4 * (levels - 1) + group) * block, block)
            qhi_ref[rows] = hi
            qlo_ref[rows] = lo
    both = jnp.concatenate(split2(b_ref[...]), axis=0)
    write_projection(msg_ref, own_ref, qhi_ref[...], qlo_ref[...], both, levels, rhs)


def near_kernel(b_ref, d_ref, near_ref, tail_ref, dhi_ref, dlo_ref):
    rhs, leaf = b_ref.shape
    chunk = 256
    field = b_ref[...]
    field_hi, field_lo = split2(field)
    both = jnp.concatenate([field_hi, field_lo], axis=0)
    for n in range(leaf // chunk):
        cols = pl.ds(n * chunk, chunk)
        d_hi, d_lo = split2(d_ref[:, cols])
        dhi_ref[:, cols] = d_hi
        dlo_ref[:, cols] = d_lo
        near_ref[:, cols] = near_product(both, field_hi, dhi_ref[:, cols], dlo_ref[:, cols], rhs)
    write_tail(tail_ref, field, near_ref[...])


def step_kernel(zero_ref, own_ref, other_ref, b_ref, near_ref, qhi_ref, qlo_ref, r_ref, image_ref, msg_ref, mine_ref):
    rhs = b_ref.shape[0]
    levels = mine_ref.shape[0] // (qhi_ref.shape[0] // 4 - mine_ref.shape[0]) + 1
    norm, product = scalars(own_ref, other_ref, rhs)
    alpha = norm / product
    far = far_product(zero_ref, own_ref, other_ref, qhi_ref[...], qlo_ref[...], rhs)
    image = near_ref[...] + far
    image_ref[...] = image
    field = b_ref[...] - alpha * image
    r_ref[...] = field
    both = jnp.concatenate(split2(field), axis=0)
    write_projection(msg_ref, mine_ref, qhi_ref[...], qlo_ref[...], both, levels, rhs)


def again_kernel(r_ref, dhi_ref, dlo_ref, near_ref, tail_ref):
    rhs = r_ref.shape[0]
    field = r_ref[...]
    field_hi, field_lo = split2(field)
    both = jnp.concatenate([field_hi, field_lo], axis=0)
    near = near_product(both, field_hi, dhi_ref[...], dlo_ref[...], rhs)
    near_ref[...] = near
    write_tail(tail_ref, field, near)


def last_kernel(order_ref, zero_ref, own_ref, other_ref, old_own_ref, old_other_ref, b_ref, image_ref, r_ref, near_ref,
                qhi_ref, qlo_ref, x_out, r_out):
    rhs, leaf = b_ref.shape
    norm_old, product_old = scalars(old_own_ref, old_other_ref, rhs)
    alpha_old = norm_old / product_old
    norm, product = scalars(own_ref, other_ref, rhs)
    ratio = norm / norm_old
    alpha = norm / (product - ratio * norm / alpha_old)
    far = far_product(zero_ref, own_ref, other_ref, qhi_ref[...], qlo_ref[...], rhs)
    direction = r_ref[...] + ratio * b_ref[...]
    along = near_ref[...] + far + ratio * image_ref[...]
    x = alpha_old * b_ref[...] + alpha * direction
    r = r_ref[...] - alpha * along
    four = jnp.concatenate(split2(x) + split2(r), axis=0)
    chunk = 256
    local_order = lax.rem(order_ref[...], leaf)
    for n in range(leaf // chunk):
        cols = pl.ds(n * chunk, chunk)
        index = iota((chunk, leaf), 0) + n * chunk
        onehot = jnp.where(index == local_order, 1.0, 0.0).astype(BF16)
        got = dot_nt(four, onehot)
        x_out[:, cols] = got[:rhs] + got[rhs:2 * rhs]
        r_out[:, cols] = got[2 * rhs:3 * rhs] + got[3 * rhs:]


def swapped(value, mask):
    mask = mask ^ (mask.bit_count() & 1 if mask > 1 else 0)
    count = lax.axis_size("wide") * lax.axis_size("narrow")
    return lax.ppermute(value, AXES, [(source, source ^ mask) for source in range(count)])


def column_products(left, right):
    return jnp.sum(left * right, axis=0, keepdims=True)


def with_row(merged, row, place):
    return merged + jnp.pad(row, ((merged.shape[0] - TAIL + place, TAIL - place - 1), (0, 0)))


def butterfly(first, own, tail_of, levels, rank):
    half, part = rank // 2, rank // 4
    got = swapped(first, 1)
    tail = with_row(tail_of(), column_products(first[:half], got[:half]), 1)
    message = jnp.concatenate([own + got[half:], tail])
    parts = []
    level = 1
    low = lax.axis_size("narrow").bit_length() - 1
    while level < levels:
        if level < low or level + 1 == levels:
            other = swapped(message, 2**level)
            parts.append(other[:part])
            cross = 2.0 * column_products(message[:part], other[:part])
            message = with_row(message[part:] + other[part:], cross, 2)
            level += 1
        else:
            x = swapped(message, 2**level)
            y = swapped(message, 2 * 2**level)
            z = swapped(message, 3 * 2**level)
            far = y + z
            pair = message[part:] + x[part:]
            parts += [x[:part], far[part:2 * part]]
            cross = column_products(message[:part], x[:part]) + column_products(y[:part], z[:part])
            cross = 2.0 * (cross + column_products(pair[:part], far[part:2 * part]))
            message = with_row(pair[part:] + far[2 * part:], cross, 2)
            level += 2
    mine = jnp.concatenate(parts + [message])
    return got, mine, swapped(mine, 1)


def call(kernel, name, outs, in_specs, scratch=(), flops=0):
    return pl.pallas_call(
        kernel,
        out_shape=outs,
        in_specs=in_specs,
        out_specs=tuple(VMEM for _ in outs),
        scratch_shapes=list(scratch),
        compiler_params=pltpu.CompilerParams(vmem_limit_bytes=32 * 1024 * 1024),
        cost_estimate=pl.CostEstimate(flops=flops, bytes_accessed=0, transcendentals=0) if flops else None,
        name=name,
    )


def local(right_side, leaf_blocks, factors, leaf_order):
    leaf = leaf_blocks.shape[1]
    levels, rank, _ = factors.shape
    rhs = right_side.shape[0]
    lanes = 2 * rhs
    rows = (levels - 1) * rank // 4
    pinned = [pltpu.with_memory_space_constraint(value, pltpu.HBM) for value in (leaf_order.reshape(1, leaf), right_side, factors)]
    field = jax.ShapeDtypeStruct((rhs, leaf), F32)
    message = jax.ShapeDtypeStruct((rank // 2 + rows, lanes), F32)
    own = jax.ShapeDtypeStruct((rows, lanes), F32)
    tail = jax.ShapeDtypeStruct((TAIL, lanes), F32)
    matrix = jax.ShapeDtypeStruct((leaf, leaf), BF16)
    basis = jax.ShapeDtypeStruct((levels * rank, leaf), BF16)
    scratch = [pltpu.VMEM(right_side.shape, F32), pltpu.VMEM(factors.shape, F32), pltpu.SemaphoreType.DMA((3,))]
    b, first, mine, qhi, qlo, order = call(
        start_kernel, "start", (field, message, own, basis, basis, jax.ShapeDtypeStruct((1, leaf), jnp.int32)),
        [HBM] * 3, scratch, FLOPS)(*pinned)
    kept = {}

    def first_tail():
        kept["near"], value, kept["dhi"], kept["dlo"] = call(
            near_kernel, "near", (field, tail, matrix, matrix), [VMEM] * 2, flops=FLOPS)(b, leaf_blocks)
        return value

    zero, ours, theirs = butterfly(first, mine, first_tail, levels, rank)
    r, image, first, mine = call(step_kernel, "step", (field, field, message, own), [VMEM] * 7)(
        zero, ours, theirs, b, kept["near"], qhi, qlo)

    def next_tail():
        kept["next"], value = call(again_kernel, "again", (field, tail), [VMEM] * 3, flops=FLOPS)(r, kept["dhi"], kept["dlo"])
        return value

    zero, ours_next, theirs_next = butterfly(first, mine, next_tail, levels, rank)
    return call(last_kernel, "last", (field, field), [VMEM] * 12)(
        order, zero, ours_next, theirs_next, ours, theirs, b, image, r, kept["next"], qhi, qlo)


def solution(mesh):
    placed = (
        P(None, AXES),
        P(AXES, None),
        P(None, None, AXES),
        P(AXES),
    )
    return jax.shard_map(
        local,
        mesh=mesh,
        in_specs=placed,
        out_specs=(P(None, AXES), P(None, AXES)),
        check_vma=False,
    )
```
